32 devices in a mesh: dp: 4 (over y, x), expert: 4 (over z), tensor: 2 (over core).
Axes of the slice: x: 2, y: 2, z: 4, core: 2. Of those that a mesh axis runs over, the one named last changes fastest.
Arguments:
- tokens: bfloat16 [1, 256, 3584], P(None, ('dp', 'expert'), 'tensor'), may hold values from -6 to 6
- gate_weight: bfloat16 [16, 3584, 1024], P(('dp', 'expert'), None, 'tensor'), may hold values from -0.09375 to 0.09375
- up_weight: bfloat16 [16, 3584, 1024], P(('dp', 'expert'), None, 'tensor'), may hold values from -0.09375 to 0.09375
- down_weight: bfloat16 [16, 1024, 3584], P(('dp', 'expert'), 'tensor'), may hold values from -0.1875 to 0.1875
- expert_ids: int32 [1, 256, 8], P(None, ('dp', 'expert')), may hold values from 0 to 15, all different within a row; in each aligned block of 16 rows (0 to 15, 16 to 31, ..., all dimensions but the last counted through in order) at most 16 rows name the same one
- gate_codes: int32 [1, 256, 8], P(None, ('dp', 'expert')), may hold values from 1 to 32767
Outputs:
- mixed: bfloat16 [1, 256, 3584], P(None, ('dp', 'expert'), 'tensor')
The draws below stay inside these ranges and needn't reach their ends.
Inputs may be any that keep to these rules, and one draw needn't show every extreme that they name: `expert_ids`: the 8 experts of one token differ. For every step, of the 16 tokens that one index of dp+expert holds, no expert is named by more than 16.
All inputs are finite; a program needn't handle non-finite values.
Results may differ from the reference program's by a relative error of at most 0.0095.
Values may be sent and summed in bfloat16 or wider, within the bound.
No kernel may reach another device: no remote copies, remote signals or barrier semaphores. Data moves between devices by JAX's collectives and lax.ppermute only.
A program may use at most 64 MiB of HBM per device.

```python
import math
import jax
import jax.numpy as jnp
import numpy as np
from jax import lax

D = 3584
FF = 1024
TOP = 8
STEPS = 1
TOK = 16
EXPERTS = 16
MOST = 16
TOKENS = 256
N_DP = 4
N_EXPERT = 4
N_TENSOR = 2


def with_ends(array, own_key, smallest, high):
    place = [jax.random.randint(jax.random.fold_in(own_key, axis), (), 0, length) for axis, length in enumerate(array.shape)]
    main_axis = array.shape.index(max(array.shape))
    beside = place[:main_axis] + [(place[main_axis] + 1) % array.shape[main_axis]] + place[main_axis + 1:]
    return array.at[tuple(place)].set(smallest).at[tuple(beside)].set(high)


def steps_of(key, shape, shards, low, top_value):
    loudness, own = 1.0, jax.random.fold_in(key, 6)
    for position, parts in shards:
        draws = jnp.exp(jax.random.uniform(jax.random.fold_in(own, position), (parts,), jnp.float32, low / len(shards), top_value / len(shards)))
        loudness = loudness * jnp.repeat(draws, shape[position] // parts).reshape([-1 if axis == position else 1 for axis in range(len(shape))])
    return loudness


def shared_out(stream_key, own, number, rows, number_of, top, bound, skew):
    ranking = jax.random.permutation(stream_key, number_of)
    crowded, common = load_shares(number_of, rows * top, bound, skew, True), load_shares(number_of, rows * top, bound, skew, False)
    places = jnp.arange(number_of)

    def named(tallies, rotation):
        used = int((tallies > 0).sum())
        fixed = max(1, used // 4)
        moved = fixed + (places - fixed + rotation * (used - fixed)) % max(1, number_of - fixed)
        return jnp.zeros((number_of,), jnp.int32).at[ranking[jnp.where(places < fixed, places, moved)]].set(jnp.asarray(tallies, jnp.int32))

    tallies = jnp.where(number % 4 == 0, named(crowded, number // 4), named(common, number - number // 4 - 1))
    mixed = jax.random.permutation(jax.random.fold_in(own, 3), number_of)
    source_of, taker = mixed[0:number_of // 2 * 2:2], mixed[1:number_of // 2 * 2:2]
    margin = jnp.minimum(tallies[source_of] - 1, bound - tallies[taker]) // 2
    margin = jnp.where((source_of == ranking[0]) | (taker == ranking[0]) | (tallies[taker] == 0), 0, jnp.maximum(margin, 0))
    moved = jax.random.randint(jax.random.fold_in(own, 4), (number_of // 2,), 0, 1 << 20) % (margin + 1)
    tallies = tallies.at[source_of].add(-moved).at[taker].add(moved)
    members = jnp.searchsorted(jnp.cumsum(tallies), jnp.arange(rows * top), side="right").astype(jnp.int32)
    grid = members.reshape(top, rows).T
    grid = grid[jax.random.permutation(jax.random.fold_in(own, 1), rows)]
    rotation = jax.random.randint(jax.random.fold_in(own, 2), (rows, 1), 0, top)
    return jnp.take_along_axis(grid, (jnp.arange(top)[None, :] + rotation) % top, axis=1)


def load_shares(amount, total, bound, slope, full):
    weights = [(1 << 20) // math.isqrt(grade ** slope) + 1 for grade in range(1, amount + 1)]
    largest = bound if full else min(bound, max(-(-total // amount), total * weights[0] // sum(weights)))
    least = 1 if total - largest >= amount - 1 else 0
    given, spare = [largest] + [least] * (amount - 1), total - largest - least * (amount - 1)
    while spare > 0:
        free = [i for i in range(1, amount) if given[i] < largest] or [i for i in range(1, amount) if given[i] < bound]
        pool, left = sum([weights[i] for i in free]), spare
        for i in free:
            extra = min(bound - given[i], max(1, left * weights[i] // pool), spare)
            given[i] = given[i] + extra
            spare = spare - extra
    return np.array(given)


def noise(own_key, extent, spread, bound, shards=(), kind=jnp.bfloat16):
    level = steps_of(own_key, extent, shards, -0.22, 0.18) if shards else 1.0
    values = jax.random.normal(own_key, extent, jnp.float32) * spread * level
    return jnp.minimum(jnp.maximum(values, -bound), bound).astype(kind)


def setup_inputs(seed: int = 0) -> dict:
    keys = jax.random.split(jax.random.key(seed), 7)
    tokens = noise(keys[0], (STEPS, TOKENS, D), 1.0, 6.0, ((1, 16), (2, 2)))
    gate_weight = noise(keys[1], (EXPERTS, D, FF), D ** -0.5, 0.09375, ((0, 16), (2, 2)))
    up_weight = noise(keys[2], (EXPERTS, D, FF), D ** -0.5, 0.09375, ((0, 16), (2, 2)))
    down_weight = noise(keys[3], (EXPERTS, FF, D), FF ** -0.5, 0.1875, ((0, 16), (1, 2)))
    expert_ids_keys = jax.random.split(jax.random.fold_in(keys[4], 1), STEPS * TOKENS // TOK)
    expert_ids_turns = jax.random.permutation(jax.random.fold_in(keys[4], 3), STEPS * TOKENS // TOK)
    expert_ids = jax.vmap(lambda own, number: shared_out(jax.random.fold_in(keys[4], 2), own, number, TOK, EXPERTS, TOP, MOST, 2))(expert_ids_keys, expert_ids_turns).reshape((STEPS, TOKENS, TOP))
    gate_codes = with_ends(jax.random.randint(keys[5], (STEPS, TOKENS, TOP), 1, 32768), jax.random.fold_in(keys[5], 1), 1, 32767).astype(jnp.int32)
    return {"tokens": tokens, "gate_weight": gate_weight, "up_weight": up_weight, "down_weight": down_weight, "expert_ids": expert_ids, "gate_codes": gate_codes}


def reference(tokens, gate_weight, up_weight, down_weight, expert_ids, gate_codes):
    pair_count = STEPS * TOKENS * TOP
    flat_tokens = tokens.reshape(STEPS * TOKENS, D)
    flat_ids = expert_ids.reshape(pair_count).astype(jnp.int32)
    codes = gate_codes.astype(jnp.float32)
    shares = (codes / jnp.sum(codes, axis=2, keepdims=True)).reshape(pair_count)
    capacity = STEPS * N_DP * N_EXPERT * MOST
    half_units = FF // N_TENSOR

    def one_expert(expert, total):
        chosen = jnp.nonzero(flat_ids == expert, size=capacity, fill_value=pair_count)[0].astype(jnp.int32)
        valid = chosen < pair_count
        clipped = jnp.minimum(chosen, pair_count - 1).astype(jnp.int32)
        token_rows = (clipped // TOP).astype(jnp.int32)
        inputs = flat_tokens[token_rows]
        w_gate = lax.dynamic_index_in_dim(gate_weight, expert, 0, keepdims=False)
        w_up = lax.dynamic_index_in_dim(up_weight, expert, 0, keepdims=False)
        w_down = lax.dynamic_index_in_dim(down_weight, expert, 0, keepdims=False)
        gated = jnp.dot(inputs, w_gate, preferred_element_type=jnp.float32)
        lifted = jnp.dot(inputs, w_up, preferred_element_type=jnp.float32)
        hidden = (jax.nn.silu(gated) * lifted).astype(jnp.bfloat16)
        summed = jnp.zeros((capacity, D), jnp.float32)
        for group in range(N_TENSOR):
            piece = jnp.dot(hidden[:, group * half_units:(group + 1) * half_units],
                            w_down[group * half_units:(group + 1) * half_units],
                            preferred_element_type=jnp.float32)
            summed = summed + lax.optimization_barrier(piece.astype(jnp.bfloat16)).astype(jnp.float32)
        expert_out = lax.optimization_barrier(summed.astype(jnp.bfloat16)).astype(jnp.float32)
        scale = jnp.where(valid, shares[clipped], jnp.zeros((capacity,), jnp.float32))
        return total.at[token_rows].add(scale[:, None] * expert_out)

    total = lax.fori_loop(0, N_DP * N_EXPERT, one_expert, jnp.zeros((STEPS * TOKENS, D), jnp.float32))
    return total.astype(jnp.bfloat16).reshape(STEPS, TOKENS, D)
```

```python
import functools

import jax
import jax.numpy as jnp
from jax import lax
from jax.experimental import pallas as pl
from jax.experimental.pallas import tpu as pltpu
from jax.sharding import PartitionSpec as P


LANES = 128


def slotted(tokens, gate_weight, up_weight, down_weight, expert_ids, gate_codes, slot_depth):
    owners = lax.axis_size("dp") * lax.axis_size("expert")
    tok_rows = tokens.shape[1]
    top_count = expert_ids.shape[2]
    slot_count = owners * slot_depth
    w_gate = gate_weight[0]
    w_up = up_weight[0]
    w_down = down_weight[0]
    slot_numbers = jnp.arange(slot_count, dtype=jnp.int32)
    owner_numbers = jnp.arange(owners, dtype=jnp.int32)
    step_tokens = tokens[0]
    route_ids = expert_ids[0].reshape(tok_rows * top_count)
    onehot = (route_ids[:, None] == owner_numbers[None, :]).astype(jnp.int32)
    before = jnp.cumsum(onehot, axis=0) - onehot
    slot_rank = jnp.sum(before * onehot, axis=1)
    slot_index = route_ids * slot_depth + slot_rank
    select = (slot_index[:, None] == slot_numbers[None, :]).astype(jnp.bfloat16)
    per_token = jnp.sum(select.reshape(tok_rows, top_count, slot_count), axis=1)
    packed = jnp.einsum(
        "ts,td->sd", per_token, step_tokens, preferred_element_type=jnp.float32
    ).astype(jnp.bfloat16)
    packed = packed.reshape(owners, slot_depth, step_tokens.shape[1])
    arrived = lax.all_to_all(packed, ("dp", "expert"), split_axis=0, concat_axis=0, tiled=True)
    owner_rows = arrived.reshape(slot_count, step_tokens.shape[1])
    owner_rows = lax.all_gather(owner_rows, "tensor", axis=1, tiled=True)
    gated = jnp.dot(owner_rows, w_gate, preferred_element_type=jnp.float32)
    lifted = jnp.dot(owner_rows, w_up, preferred_element_type=jnp.float32)
    hidden = (jax.nn.silu(gated) * lifted).astype(jnp.bfloat16)
    partial_value = jnp.dot(hidden, w_down, preferred_element_type=jnp.float32).astype(jnp.bfloat16)
    summed = (
        lax.psum_scatter(partial_value, "tensor", scatter_dimension=1, tiled=True)
        .astype(jnp.float32)
        .astype(jnp.bfloat16)
    )
    half_width = summed.shape[1]
    result = summed.reshape(owners, slot_depth, half_width)
    returned = lax.all_to_all(result, ("dp", "expert"), split_axis=0, concat_axis=0, tiled=True)
    returned = returned.reshape(slot_count, half_width)
    picked = jnp.dot(select, returned, preferred_element_type=jnp.float32)
    codes = gate_codes[0].astype(jnp.float32)
    shares = codes / jnp.sum(codes, axis=1, keepdims=True)
    mixed_rows = jnp.sum(
        picked.reshape(tok_rows, top_count, half_width) * shares[:, :, None], axis=1
    )
    return mixed_rows.astype(jnp.bfloat16)[None]


def swap(x, axis, offset):
    count = lax.axis_size(axis)
    return lax.ppermute(x, axis, [(i, i ^ offset) for i in range(count)])


def prepare(owners, tok_ref, ids_ref, codes_ref, out_ref):
    width = tok_ref.shape[1]
    rows = tok_ref.shape[0]
    top_count = ids_ref.shape[0]
    out_ref[:, :width] = tok_ref[...]
    ids = jnp.transpose(ids_ref[...])
    codes = jnp.transpose(codes_ref[...].astype(jnp.float32))
    shares = codes / jnp.sum(codes, axis=1, keepdims=True)
    lane = lax.broadcasted_iota(jnp.int32, (rows, LANES), 1)
    expert = lax.rem(lane, owners)
    dense = jnp.zeros((rows, LANES), jnp.float32)
    for k in range(top_count):
        dense += jnp.where(ids[:, k : k + 1] == expert, shares[:, k : k + 1], 0.0)
    high = dense.astype(jnp.bfloat16)
    low = (dense - high.astype(jnp.float32)).astype(jnp.bfloat16)
    zero = jnp.zeros_like(high)
    out_ref[:, width:] = jnp.where(lane < owners, high, jnp.where(lane < 2 * owners, low, zero))


def expert_ffn(groups, owners, *refs):
    own = refs[:groups]
    other = refs[groups : 2 * groups]
    gate_ref, up_ref, down_ref = refs[2 * groups : 2 * groups + 3]
    keep = refs[2 * groups + 3 : 3 * groups + 3]
    send = refs[3 * groups + 3 : 4 * groups + 3]
    x_own, x_other, hidden_ref = refs[4 * groups + 3 :]
    rows = own[0].shape[0]
    width = own[0].shape[1] - LANES
    hidden_units = gate_ref.shape[1]
    half = lax.axis_index("tensor")
    expert = lax.axis_index("dp") * lax.axis_size("expert") + lax.axis_index("expert")
    for g in range(groups):
        x_own[pl.ds(g * rows, rows), :] = own[g][:, :width]
        x_other[pl.ds(g * rows, rows), :] = other[g][:, :width]
    first = pl.multiple_of(half * width, LANES)
    second = pl.multiple_of((1 - half) * width, LANES)
    tile = 256

    def dot(a, b):
        return jnp.dot(a, b, preferred_element_type=jnp.float32)

    @pl.loop(0, hidden_units // tile)
    def _(i):
        columns = pl.ds(pl.multiple_of(i * tile, tile), tile)
        a, b = x_own[...], x_other[...]
        gated = dot(a, gate_ref[pl.ds(first, width), columns]) + dot(b, gate_ref[pl.ds(second, width), columns])
        lifted = dot(a, up_ref[pl.ds(first, width), columns]) + dot(b, up_ref[pl.ds(second, width), columns])
        hidden_ref[:, columns] = (jax.nn.silu(gated) * lifted).astype(jnp.bfloat16)

    scales = []
    for g in range(groups):
        lane = lax.broadcasted_iota(jnp.int32, (rows, LANES), 1)
        mine = (lane == expert) | (lane == expert + owners)
        scales.append(jnp.sum(jnp.where(mine, own[g][:, width:].astype(jnp.float32), 0.0), axis=1, keepdims=True))

    @pl.loop(0, width // tile)
    def _(i):
        columns = pl.ds(pl.multiple_of(i * tile, tile), tile)
        h = hidden_ref[...]
        for start, outs in ((second, send), (first, keep)):
            value = dot(h, down_ref[:, pl.ds(pl.multiple_of(start + i * tile, LANES), tile)])
            for g in range(groups):
                outs[g][:, columns] = (value[g * rows : (g + 1) * rows] * scales[g]).astype(jnp.bfloat16)


def dense(tokens, gate_weight, up_weight, down_weight, expert_ids, gate_codes):
    dp, ex = lax.axis_size("dp"), lax.axis_size("expert")
    owners = dp * ex
    tok_rows, width = tokens.shape[1:]
    bf16 = jnp.bfloat16
    payload = pl.pallas_call(
        functools.partial(prepare, owners),
        out_shape=jax.ShapeDtypeStruct((tok_rows, width + LANES), bf16),
        name="prepare",
    )(tokens[0], expert_ids[0].T, gate_codes[0].T)
    line = jnp.concatenate([payload] + [swap(payload, "expert", j) for j in range(1, ex)], axis=0)
    own = [line] + [swap(line, "dp", g) for g in range(1, dp)]
    other = [swap(x, "tensor", 1) for x in own]
    rows = ex * tok_rows
    vmem = pl.BlockSpec(memory_space=pltpu.VMEM)
    anyspace = pl.BlockSpec(memory_space=pl.ANY)
    out = jax.ShapeDtypeStruct((rows, width), bf16)
    hidden_units = gate_weight.shape[2]
    flops = 2 * dp * rows * 3 * 2 * width * hidden_units
    results = pl.pallas_call(
        functools.partial(expert_ffn, dp, owners),
        in_specs=[vmem] * (2 * dp) + [vmem] * 3,
        out_specs=[vmem] * (2 * dp),
        out_shape=[out] * (2 * dp),
        scratch_shapes=[
            pltpu.VMEM((dp * rows, width), bf16),
            pltpu.VMEM((dp * rows, width), bf16),
            pltpu.VMEM((dp * rows, hidden_units), bf16),
        ],
        cost_estimate=pl.CostEstimate(flops=flops, bytes_accessed=3 * 2 * 2 * width * hidden_units, transcendentals=0),
        name="expert_ffn",
    )(*own, *other, gate_weight[0], up_weight[0], down_weight[0])
    keep, send = results[:dp], results[dp:]
    f32 = jnp.float32
    order = list(range(dp - 1, -1, -1))
    crossed = {g: swap(send[g], "tensor", 1) for g in order}
    summed = {g: keep[g].astype(f32) + crossed[g].astype(f32) for g in order}
    moved = {g: swap(summed[g].astype(bf16), "dp", g) for g in order if g}
    total = summed[0]
    for g in moved:
        total = total + moved[g].astype(f32)
    parts = [total[j * tok_rows : (j + 1) * tok_rows] for j in range(ex)]
    final = parts[0]
    for j in range(ex - 1, 0, -1):
        final = final + swap(parts[j].astype(bf16), "expert", j).astype(f32)
    return final.astype(bf16)[None]


def local(tokens, gate_weight, up_weight, down_weight, expert_ids, gate_codes):
    dp, ex = lax.axis_size("dp"), lax.axis_size("expert")
    owners = dp * ex
    tok_rows = tokens.shape[1]
    top_count = expert_ids.shape[2]
    slot_depth = min(tok_rows, max(2, 2 * tok_rows * top_count // owners))
    args = (tokens, gate_weight, up_weight, down_weight, expert_ids, gate_codes)
    powers = dp & (dp - 1) == 0 and ex & (ex - 1) == 0 and lax.axis_size("tensor") == 2
    if slot_depth == tok_rows and powers and 2 * owners <= LANES:
        return dense(*args)
    return slotted(*args, slot_depth)


def solution(mesh):
    in_specs = (
        P(None, ("dp", "expert"), "tensor"),
        P(("dp", "expert"), None, "tensor"),
        P(("dp", "expert"), None, "tensor"),
        P(("dp", "expert"), "tensor", None),
        P(None, ("dp", "expert"), None),
        P(None, ("dp", "expert"), None),
    )
    out_specs = P(None, ("dp", "expert"), "tensor")
    return jax.shard_map(local, mesh=mesh, in_specs=in_specs, out_specs=out_specs, check_vma=False)
```

```python
import functools

import jax
import jax.numpy as jnp
from jax import lax
from jax.experimental import pallas as pl
from jax.experimental.pallas import tpu as pltpu
from jax.sharding import PartitionSpec as P


LANES = 128
STALL = 20000000000


def slotted(tokens, gate_weight, up_weight, down_weight, expert_ids, gate_codes, slot_depth):
    owners = lax.axis_size("dp") * lax.axis_size("expert")
    tok_rows = tokens.shape[1]
    top_count = expert_ids.shape[2]
    slot_count = owners * slot_depth
    w_gate = gate_weight[0]
    w_up = up_weight[0]
    w_down = down_weight[0]
    slot_numbers = jnp.arange(slot_count, dtype=jnp.int32)
    owner_numbers = jnp.arange(owners, dtype=jnp.int32)
    step_tokens = tokens[0]
    route_ids = expert_ids[0].reshape(tok_rows * top_count)
    onehot = (route_ids[:, None] == owner_numbers[None, :]).astype(jnp.int32)
    before = jnp.cumsum(onehot, axis=0) - onehot
    slot_rank = jnp.sum(before * onehot, axis=1)
    slot_index = route_ids * slot_depth + slot_rank
    select = (slot_index[:, None] == slot_numbers[None, :]).astype(jnp.bfloat16)
    per_token = jnp.sum(select.reshape(tok_rows, top_count, slot_count), axis=1)
    packed = jnp.einsum(
        "ts,td->sd", per_token, step_tokens, preferred_element_type=jnp.float32
    ).astype(jnp.bfloat16)
    packed = packed.reshape(owners, slot_depth, step_tokens.shape[1])
    arrived = lax.all_to_all(packed, ("dp", "expert"), split_axis=0, concat_axis=0, tiled=True)
    owner_rows = arrived.reshape(slot_count, step_tokens.shape[1])
    owner_rows = lax.all_gather(owner_rows, "tensor", axis=1, tiled=True)
    gated = jnp.dot(owner_rows, w_gate, preferred_element_type=jnp.float32)
    lifted = jnp.dot(owner_rows, w_up, preferred_element_type=jnp.float32)
    hidden = (jax.nn.silu(gated) * lifted).astype(jnp.bfloat16)
    partial_value = jnp.dot(hidden, w_down, preferred_element_type=jnp.float32).astype(jnp.bfloat16)
    summed = (
        lax.psum_scatter(partial_value, "tensor", scatter_dimension=1, tiled=True)
        .astype(jnp.float32)
        .astype(jnp.bfloat16)
    )
    half_width = summed.shape[1]
    result = summed.reshape(owners, slot_depth, half_width)
    returned = lax.all_to_all(result, ("dp", "expert"), split_axis=0, concat_axis=0, tiled=True)
    returned = returned.reshape(slot_count, half_width)
    picked = jnp.dot(select, returned, preferred_element_type=jnp.float32)
    codes = gate_codes[0].astype(jnp.float32)
    shares = codes / jnp.sum(codes, axis=1, keepdims=True)
    mixed_rows = jnp.sum(
        picked.reshape(tok_rows, top_count, half_width) * shares[:, :, None], axis=1
    )
    return mixed_rows.astype(jnp.bfloat16)[None]


def swap(x, axis, offset):
    count = lax.axis_size(axis)
    return lax.ppermute(x, axis, [(i, i ^ offset) for i in range(count)])


TILE = 256
VMEM = pl.BlockSpec(memory_space=pltpu.VMEM)
F32, BF16 = jnp.float32, jnp.bfloat16


def call(body, outs, *args, flops=0, scratch=(), limit=2):
    return pl.pallas_call(
        body,
        out_shape=outs,
        in_specs=[VMEM] * len(args),
        out_specs=jax.tree.map(lambda _: VMEM, outs),
        scratch_shapes=scratch,
        compiler_params=pltpu.CompilerParams(vmem_limit_bytes=limit * 2**20),
        cost_estimate=pl.CostEstimate(flops=flops, bytes_accessed=0, transcendentals=0),
    )(*args)


def table(owners, out_ref):
    out_ref[...] = lax.rem(lax.broadcasted_iota(jnp.int32, out_ref.shape, 1), owners)


def prepare(owners, tok_ref, ids_ref, codes_ref, expert_ref, out_ref):
    width = tok_ref.shape[1]
    rows = tok_ref.shape[0]
    top_count = ids_ref.shape[0]
    out_ref[:, :width] = tok_ref[...]
    ids = jnp.transpose(ids_ref[...])
    codes = jnp.transpose(codes_ref[...].astype(F32))
    shares = codes / jnp.sum(codes, axis=1, keepdims=True)
    lane = lax.broadcasted_iota(jnp.int32, (rows, LANES), 1)
    expert = expert_ref[...]
    dense = jnp.zeros((rows, LANES), F32)
    for k in range(top_count):
        dense += jnp.where(ids[:, k : k + 1] == expert, shares[:, k : k + 1], 0.0)
    high = dense.astype(BF16)
    low = (dense - high.astype(F32)).astype(BF16)
    out_ref[:, width:] = jnp.where(lane < owners, high, jnp.where(lane < 2 * owners, low, jnp.zeros_like(high)))


def stack(blocks, flops=0):
    def body(*refs):
        start = 0
        for ref in refs[:-1]:
            refs[-1][start : start + ref.shape[0], :] = ref[...]
            start += ref.shape[0]

    rows = sum(b.shape[0] for b in blocks)
    return call(body, jax.ShapeDtypeStruct((rows, blocks[0].shape[1]), BF16), *blocks, flops=flops)


def dot(a, b):
    return jnp.dot(a, b, preferred_element_type=F32)


def plus(*values):
    total = values[0].astype(F32)
    for value in values[1:]:
        total = total + value.astype(F32)
    return total


def ffn(groups, owners, *refs):
    own, other = refs[:groups], refs[groups : 2 * groups]
    gate, up, down = refs[2 * groups : 2 * groups + 3]
    keep, send = refs[2 * groups + 3 : 3 * groups + 3], refs[3 * groups + 3 : 4 * groups + 3]
    x_own, x_other, hidden = refs[4 * groups + 3 :]
    rows, width = keep[0].shape
    half = lax.axis_index("tensor")
    expert = lax.axis_index("dp") * lax.axis_size("expert") + lax.axis_index("expert")
    first = pl.ds(pl.multiple_of(half * width, LANES), width)
    second = pl.ds(pl.multiple_of((1 - half) * width, LANES), width)
    scales = []
    for g in range(groups):
        there = pl.ds(g * rows, rows)
        x_own[there, :] = own[g][:, :width]
        x_other[there, :] = other[g][:, :width]
        lane = lax.broadcasted_iota(jnp.int32, (rows, LANES), 1)
        mine = (lane == expert) | (lane == expert + owners)
        scales.append(jnp.sum(jnp.where(mine, own[g][:, width:].astype(F32), 0.0), axis=1, keepdims=True))

    @pl.loop(0, hidden.shape[1] // TILE)
    def _(i):
        columns = pl.ds(pl.multiple_of(i * TILE, TILE), TILE)
        a, b = x_own[...], x_other[...]
        gated = dot(a, gate[first, columns]) + dot(b, gate[second, columns])
        lifted = dot(a, up[first, columns]) + dot(b, up[second, columns])
        hidden[:, columns] = (jax.nn.silu(gated) * lifted).astype(BF16)

    @pl.loop(0, width // TILE)
    def _(i):
        columns = pl.ds(pl.multiple_of(i * TILE, TILE), TILE)
        h = hidden[...]
        for start, outs in (((1 - half) * width, send), (half * width, keep)):
            value = dot(h, down[:, pl.ds(pl.multiple_of(start + i * TILE, LANES), TILE)])
            for g in range(groups):
                outs[g][:, columns] = (value[g * rows : (g + 1) * rows] * scales[g]).astype(BF16)


def dense(tokens, gate_weight, up_weight, down_weight, expert_ids, gate_codes):
    dp, ex = lax.axis_size("dp"), lax.axis_size("expert")
    owners = dp * ex
    n, width = tokens.shape[1:]
    units = gate_weight.shape[2]
    hops = range(1, ex)
    rows = ex * n

    def block(count):
        return jax.ShapeDtypeStruct((count, width), BF16)

    experts = call(functools.partial(table, owners), jax.ShapeDtypeStruct((n, LANES), jnp.int32), flops=STALL)
    first = call(
        functools.partial(prepare, owners),
        jax.ShapeDtypeStruct((n, width + LANES), BF16),
        tokens[0], expert_ids[0].T, gate_codes[0].T, experts,
    )
    line = {j: swap(first, "expert", j) for j in reversed(hops)}
    corner = swap(first, "dp", 3)
    diag = {j: swap(corner, "expert", j) for j in reversed(hops)}
    near = stack([first] + [line[j] for j in hops], flops=STALL)
    own = [near, swap(near, "dp", 1), swap(near, "dp", 2), stack([corner] + [diag[j] for j in hops], flops=STALL)]
    other = [swap(own[g], "tensor", 1) for g in range(dp)]
    weights = 3 * 2 * width * units
    results = call(
        functools.partial(ffn, dp, owners),
        [block(rows)] * (2 * dp),
        *own, *other, gate_weight[0], up_weight[0], down_weight[0],
        flops=2 * weights * dp * rows, limit=24,
        scratch=[pltpu.VMEM((dp * rows, width), BF16)] * 2 + [pltpu.VMEM((dp * rows, units), BF16)],
    )
    keep, send = results[:dp], results[dp:]
    back = {g: swap(send[g], "tensor", 1) for g in (1, 2, 3, 0)}

    def add(keep, recv, out):
        out[...] = plus(keep[...], recv[...]).astype(BF16)

    def add_split(keep, recv, *outs):
        for i, out in enumerate(outs):
            there = pl.ds((i + 1) * n, n)
            out[...] = plus(keep[there, :], recv[there, :]).astype(BF16)

    sides = {g: swap(call(add, block(rows), keep[g], back[g]), "dp", g) for g in (1, 2)}
    parts = call(add_split, [block(n)] * (ex - 1), keep[3], back[3])
    spread = [swap(parts[j - 1], "expert", j) for j in reversed(hops)]

    def add_diag(keep, recv, *rest):
        here = pl.ds(0, n)
        rest[-1][...] = plus(keep[here, :], recv[here, :], *[r[...] for r in rest[:-1]]).astype(BF16)

    def add_line(keep, recv, x, y, *outs):
        for i, out in enumerate(outs):
            there = pl.ds((i + 1) * n, n)
            out[...] = plus(keep[there, :], recv[there, :], x[there, :], y[there, :]).astype(BF16)

    lines = call(add_line, [block(n)] * (ex - 1), keep[0], back[0], sides[1], sides[2])
    ends = [swap(lines[j - 1], "expert", j) for j in reversed(hops)]
    turned = call(add_diag, block(n), keep[3], back[3], *spread)
    ends.append(swap(turned, "dp", 3))

    def add_end(keep, recv, x, y, *rest):
        here = pl.ds(0, n)
        rest[-1][...] = plus(keep[here, :], recv[here, :], x[here, :], y[here, :], *[r[...] for r in rest[:-1]]).astype(BF16)

    return call(add_end, block(n), keep[0], back[0], sides[1], sides[2], *ends)[None]


def local(tokens, gate_weight, up_weight, down_weight, expert_ids, gate_codes):
    dp, ex = lax.axis_size("dp"), lax.axis_size("expert")
    owners = dp * ex
    tok_rows = tokens.shape[1]
    top_count = expert_ids.shape[2]
    slot_depth = min(tok_rows, max(2, 2 * tok_rows * top_count // owners))
    args = (tokens, gate_weight, up_weight, down_weight, expert_ids, gate_codes)
    grid = dp == 4 and ex & (ex - 1) == 0 and ex > 1 and lax.axis_size("tensor") == 2
    if slot_depth == tok_rows and grid and 2 * owners <= LANES:
        return dense(*args)
    return slotted(*args, slot_depth)


def solution(mesh):
    in_specs = (
        P(None, ("dp", "expert"), "tensor"),
        P(("dp", "expert"), None, "tensor"),
        P(("dp", "expert"), None, "tensor"),
        P(("dp", "expert"), "tensor", None),
        P(None, ("dp", "expert"), None),
        P(None, ("dp", "expert"), None),
    )
    out_specs = P(None, ("dp", "expert"), "tensor")
    return jax.shard_map(local, mesh=mesh, in_specs=in_specs, out_specs=out_specs, check_vma=False)
```

```python
import functools

import jax
import jax.numpy as jnp
from jax import lax
from jax.experimental import pallas as pl
from jax.experimental.pallas import tpu as pltpu
from jax.sharding import PartitionSpec as P


LANES = 128
STALL = 20000000000
EARLY = 2
TILE = 256


def slotted(tokens, gate_weight, up_weight, down_weight, expert_ids, gate_codes, slot_depth):
    owners = lax.axis_size("dp") * lax.axis_size("expert")
    tok_rows = tokens.shape[1]
    top_count = expert_ids.shape[2]
    slot_count = owners * slot_depth
    w_gate = gate_weight[0]
    w_up = up_weight[0]
    w_down = down_weight[0]
    slot_numbers = jnp.arange(slot_count, dtype=jnp.int32)
    owner_numbers = jnp.arange(owners, dtype=jnp.int32)
    step_tokens = tokens[0]
    route_ids = expert_ids[0].reshape(tok_rows * top_count)
    onehot = (route_ids[:, None] == owner_numbers[None, :]).astype(jnp.int32)
    before = jnp.cumsum(onehot, axis=0) - onehot
    slot_rank = jnp.sum(before * onehot, axis=1)
    slot_index = route_ids * slot_depth + slot_rank
    select = (slot_index[:, None] == slot_numbers[None, :]).astype(jnp.bfloat16)
    per_token = jnp.sum(select.reshape(tok_rows, top_count, slot_count), axis=1)
    packed = jnp.einsum(
        "ts,td->sd", per_token, step_tokens, preferred_element_type=jnp.float32
    ).astype(jnp.bfloat16)
    packed = packed.reshape(owners, slot_depth, step_tokens.shape[1])
    arrived = lax.all_to_all(packed, ("dp", "expert"), split_axis=0, concat_axis=0, tiled=True)
    owner_rows = arrived.reshape(slot_count, step_tokens.shape[1])
    owner_rows = lax.all_gather(owner_rows, "tensor", axis=1, tiled=True)
    gated = jnp.dot(owner_rows, w_gate, preferred_element_type=jnp.float32)
    lifted = jnp.dot(owner_rows, w_up, preferred_element_type=jnp.float32)
    hidden = (jax.nn.silu(gated) * lifted).astype(jnp.bfloat16)
    partial_value = jnp.dot(hidden, w_down, preferred_element_type=jnp.float32).astype(jnp.bfloat16)
    summed = (
        lax.psum_scatter(partial_value, "tensor", scatter_dimension=1, tiled=True)
        .astype(jnp.float32)
        .astype(jnp.bfloat16)
    )
    half_width = summed.shape[1]
    result = summed.reshape(owners, slot_depth, half_width)
    returned = lax.all_to_all(result, ("dp", "expert"), split_axis=0, concat_axis=0, tiled=True)
    returned = returned.reshape(slot_count, half_width)
    picked = jnp.dot(select, returned, preferred_element_type=jnp.float32)
    codes = gate_codes[0].astype(jnp.float32)
    shares = codes / jnp.sum(codes, axis=1, keepdims=True)
    mixed_rows = jnp.sum(
        picked.reshape(tok_rows, top_count, half_width) * shares[:, :, None], axis=1
    )
    return mixed_rows.astype(jnp.bfloat16)[None]


def swap(x, axis, offset):
    count = lax.axis_size(axis)
    return lax.ppermute(x, axis, [(i, i ^ offset) for i in range(count)])


VMEM = pl.BlockSpec(memory_space=pltpu.VMEM)
F32, BF16 = jnp.float32, jnp.bfloat16


def call(body, outs, *args, flops=0, scratch=(), limit=2):
    return pl.pallas_call(
        body,
        out_shape=outs,
        in_specs=[VMEM] * len(args),
        out_specs=jax.tree.map(lambda _: VMEM, outs),
        scratch_shapes=scratch,
        compiler_params=pltpu.CompilerParams(vmem_limit_bytes=limit * 2**20),
        cost_estimate=pl.CostEstimate(flops=flops, bytes_accessed=0, transcendentals=0),
    )(*args)


def table(owners, out_ref):
    out_ref[...] = lax.rem(lax.broadcasted_iota(jnp.int32, out_ref.shape, 1), owners)


def prepare(owners, tok_ref, ids_ref, codes_ref, expert_ref, out_ref):
    width = tok_ref.shape[1]
    rows = tok_ref.shape[0]
    top_count = ids_ref.shape[0]
    out_ref[:, :width] = tok_ref[...]
    ids = jnp.transpose(ids_ref[...])
    codes = jnp.transpose(codes_ref[...].astype(F32))
    shares = codes / jnp.sum(codes, axis=1, keepdims=True)
    lane = lax.broadcasted_iota(jnp.int32, (rows, LANES), 1)
    expert = expert_ref[...]
    dense = jnp.zeros((rows, LANES), F32)
    for k in range(top_count):
        dense += jnp.where(ids[:, k : k + 1] == expert, shares[:, k : k + 1], 0.0)
    high = dense.astype(BF16)
    low = (dense - high.astype(F32)).astype(BF16)
    out_ref[:, width:] = jnp.where(lane < owners, high, jnp.where(lane < 2 * owners, low, jnp.zeros_like(high)))


def stack(blocks, flops=0):
    def body(*refs):
        start = 0
        for ref in refs[:-1]:
            refs[-1][start : start + ref.shape[0], :] = ref[...]
            start += ref.shape[0]

    rows = sum(b.shape[0] for b in blocks)
    return call(body, jax.ShapeDtypeStruct((rows, blocks[0].shape[1]), BF16), *blocks, flops=flops)


def dot(a, b):
    return jnp.dot(a, b, preferred_element_type=F32)


def plus(*values):
    total = values[0].astype(F32)
    for value in values[1:]:
        total = total + value.astype(F32)
    return total


def ffn(owners, own, other, gate, up, down, keep, send, x, hidden):
    rows, width = keep.shape
    half = lax.axis_index("tensor")
    expert = lax.axis_index("dp") * lax.axis_size("expert") + lax.axis_index("expert")
    mine_at = pl.ds(pl.multiple_of(half * width, LANES), width)
    other_at = pl.ds(pl.multiple_of((1 - half) * width, LANES), width)
    x[:, mine_at] = own[:, :width]
    x[:, other_at] = other[:, :width]
    lane = lax.broadcasted_iota(jnp.int32, (rows, LANES), 1)
    mine = (lane == expert) | (lane == expert + owners)
    scale = jnp.sum(jnp.where(mine, own[:, width:].astype(F32), 0.0), axis=1, keepdims=True)
    for i in range(0, hidden.shape[1], TILE):
        at = pl.ds(i, TILE)
        gated, lifted = dot(x[...], gate[:, at]), dot(x[...], up[:, at])
        hidden[:, at] = (jax.nn.silu(gated) * lifted).astype(BF16)
    for at, out in ((other_at, send), (mine_at, keep)):
        out[...] = (dot(hidden[...], down[:, at]) * scale).astype(BF16)


def dense(tokens, gate_weight, up_weight, down_weight, expert_ids, gate_codes):
    dp, ex = lax.axis_size("dp"), lax.axis_size("expert")
    owners = dp * ex
    n, width = tokens.shape[1:]
    units = gate_weight.shape[2]
    hops = range(1, ex)
    rows = ex * n

    def block(count):
        return jax.ShapeDtypeStruct((count, width), BF16)

    experts = call(functools.partial(table, owners), jax.ShapeDtypeStruct((n, LANES), jnp.int32), flops=STALL)
    first = call(
        functools.partial(prepare, owners),
        jax.ShapeDtypeStruct((n, width + LANES), BF16),
        tokens[0], expert_ids[0].T, gate_codes[0].T, experts,
    )
    line = {j: swap(first, "expert", j) for j in reversed(hops)}
    early = [first] + [line[j] for j in range(1, EARLY)]
    late = [line[j] for j in range(EARLY, ex)]
    parts_a = stack(early)
    parts_b = stack(late, flops=STALL)
    sent_a = {g: swap(parts_a, "dp", g) for g in range(1, dp)}
    sent_b = {g: swap(parts_b, "dp", g) for g in range(1, dp)}
    near = stack([parts_a, parts_b] + [sent_a[g] for g in range(1, dp)])
    far = stack([sent_b[g] for g in range(1, dp)], flops=STALL)
    matrices = gate_weight[0], up_weight[0], down_weight[0]

    def run(own):
        count = own.shape[0]
        return call(
            functools.partial(ffn, owners),
            [block(count)] * 2,
            own, swap(own, "tensor", 1), *matrices,
            flops=STALL, limit=16,
            scratch=[pltpu.VMEM((count, 2 * width), BF16), pltpu.VMEM((count, units), BF16)],
        )

    keep_a, send_a = run(near)
    keep_b, send_b = run(far)
    recv_a = swap(send_a, "tensor", 1)
    recv_b = swap(send_b, "tensor", 1)
    cut = EARLY * n

    def add_far(keep_a, recv_a, keep_b, recv_b, x, y, *diag):
        for g, out in ((1, x), (2, y)):
            here, there = pl.ds(rows + (g - 1) * cut, cut), pl.ds((g - 1) * (rows - cut), rows - cut)
            out[:cut, :] = plus(keep_a[here, :], recv_a[here, :]).astype(BF16)
            out[cut:, :] = plus(keep_b[there, :], recv_b[there, :]).astype(BF16)
        for j, out in zip(hops, diag):
            if j < EARLY:
                keep, recv, here = keep_a, recv_a, pl.ds(rows + 2 * cut + j * n, n)
            else:
                keep, recv, here = keep_b, recv_b, pl.ds(2 * (rows - cut) + (j - EARLY) * n, n)
            out[...] = plus(keep[here, :], recv[here, :]).astype(BF16)

    x, y, *diag = call(add_far, [block(rows)] * 2 + [block(n)] * (ex - 1), keep_a, recv_a, keep_b, recv_b)
    sides = [swap(x, "dp", 1), swap(y, "dp", 2)]
    spread = [swap(diag[j - 1], "expert", j) for j in reversed(hops)]

    def add_diag(keep, recv, *rest):
        here = pl.ds(rows + 2 * cut, n)
        rest[-1][...] = plus(keep[here, :], recv[here, :], *[r[...] for r in rest[:-1]]).astype(BF16)

    def add_line(keep, recv, x, y, *outs):
        for i, out in enumerate(outs):
            there = pl.ds((i + 1) * n, n)
            out[...] = plus(keep[there, :], recv[there, :], x[there, :], y[there, :]).astype(BF16)

    lines = call(add_line, [block(n)] * (ex - 1), keep_a, recv_a, *sides)
    ends = [swap(lines[j - 1], "expert", j) for j in reversed(hops)]
    ends.append(swap(call(add_diag, block(n), keep_a, recv_a, *spread), "dp", 3))

    def add_end(keep, recv, x, y, *rest):
        here = pl.ds(0, n)
        rest[-1][...] = plus(keep[here, :], recv[here, :], x[here, :], y[here, :], *[r[...] for r in rest[:-1]]).astype(BF16)

    return call(add_end, block(n), keep_a, recv_a, *sides, *ends)[None]


def local(tokens, gate_weight, up_weight, down_weight, expert_ids, gate_codes):
    dp, ex = lax.axis_size("dp"), lax.axis_size("expert")
    owners = dp * ex
    tok_rows = tokens.shape[1]
    top_count = expert_ids.shape[2]
    slot_depth = min(tok_rows, max(2, 2 * tok_rows * top_count // owners))
    args = (tokens, gate_weight, up_weight, down_weight, expert_ids, gate_codes)
    grid = dp == 4 and ex & (ex - 1) == 0 and ex > 1 and lax.axis_size("tensor") == 2
    if slot_depth == tok_rows and grid and 2 * owners <= LANES:
        return dense(*args)
    return slotted(*args, slot_depth)


def solution(mesh):
    in_specs = (
        P(None, ("dp", "expert"), "tensor"),
        P(("dp", "expert"), None, "tensor"),
        P(("dp", "expert"), None, "tensor"),
        P(("dp", "expert"), "tensor", None),
        P(None, ("dp", "expert"), None),
        P(None, ("dp", "expert"), None),
    )
    out_specs = P(None, ("dp", "expert"), "tensor")
    return jax.shard_map(local, mesh=mesh, in_specs=in_specs, out_specs=out_specs, check_vma=False)
```

```python
import functools

import jax
import jax.numpy as jnp
from jax import lax
from jax.experimental import pallas as pl
from jax.experimental.pallas import tpu as pltpu
from jax.sharding import PartitionSpec as P


LANES = 128
STALL = 20000000000
EARLY = 2
TILE = 256
HINT = 2000000000


def slotted(tokens, gate_weight, up_weight, down_weight, expert_ids, gate_codes, slot_depth):
    owners = lax.axis_size("dp") * lax.axis_size("expert")
    tok_rows = tokens.shape[1]
    top_count = expert_ids.shape[2]
    slot_count = owners * slot_depth
    w_gate = gate_weight[0]
    w_up = up_weight[0]
    w_down = down_weight[0]
    slot_numbers = jnp.arange(slot_count, dtype=jnp.int32)
    owner_numbers = jnp.arange(owners, dtype=jnp.int32)
    step_tokens = tokens[0]
    route_ids = expert_ids[0].reshape(tok_rows * top_count)
    onehot = (route_ids[:, None] == owner_numbers[None, :]).astype(jnp.int32)
    before = jnp.cumsum(onehot, axis=0) - onehot
    slot_rank = jnp.sum(before * onehot, axis=1)
    slot_index = route_ids * slot_depth + slot_rank
    select = (slot_index[:, None] == slot_numbers[None, :]).astype(jnp.bfloat16)
    per_token = jnp.sum(select.reshape(tok_rows, top_count, slot_count), axis=1)
    packed = jnp.einsum(
        "ts,td->sd", per_token, step_tokens, preferred_element_type=jnp.float32
    ).astype(jnp.bfloat16)
    packed = packed.reshape(owners, slot_depth, step_tokens.shape[1])
    arrived = lax.all_to_all(packed, ("dp", "expert"), split_axis=0, concat_axis=0, tiled=True)
    owner_rows = arrived.reshape(slot_count, step_tokens.shape[1])
    owner_rows = lax.all_gather(owner_rows, "tensor", axis=1, tiled=True)
    gated = jnp.dot(owner_rows, w_gate, preferred_element_type=jnp.float32)
    lifted = jnp.dot(owner_rows, w_up, preferred_element_type=jnp.float32)
    hidden = (jax.nn.silu(gated) * lifted).astype(jnp.bfloat16)
    partial_value = jnp.dot(hidden, w_down, preferred_element_type=jnp.float32).astype(jnp.bfloat16)
    summed = (
        lax.psum_scatter(partial_value, "tensor", scatter_dimension=1, tiled=True)
        .astype(jnp.float32)
        .astype(jnp.bfloat16)
    )
    half_width = summed.shape[1]
    result = summed.reshape(owners, slot_depth, half_width)
    returned = lax.all_to_all(result, ("dp", "expert"), split_axis=0, concat_axis=0, tiled=True)
    returned = returned.reshape(slot_count, half_width)
    picked = jnp.dot(select, returned, preferred_element_type=jnp.float32)
    codes = gate_codes[0].astype(jnp.float32)
    shares = codes / jnp.sum(codes, axis=1, keepdims=True)
    mixed_rows = jnp.sum(
        picked.reshape(tok_rows, top_count, half_width) * shares[:, :, None], axis=1
    )
    return mixed_rows.astype(jnp.bfloat16)[None]


def swap(x, axis, offset):
    count = lax.axis_size(axis)
    return lax.ppermute(x, axis, [(i, i ^ offset) for i in range(count)])


VMEM = pl.BlockSpec(memory_space=pltpu.VMEM)
F32, BF16 = jnp.float32, jnp.bfloat16


def call(body, outs, *args, flops=0, scratch=(), limit=2):
    return pl.pallas_call(
        body,
        out_shape=outs,
        in_specs=[VMEM] * len(args),
        out_specs=jax.tree.map(lambda _: VMEM, outs),
        scratch_shapes=scratch,
        compiler_params=pltpu.CompilerParams(vmem_limit_bytes=limit * 2**20),
        cost_estimate=pl.CostEstimate(flops=flops, bytes_accessed=0, transcendentals=0),
    )(*args)


def table(owners, out_ref):
    out_ref[...] = lax.rem(lax.broadcasted_iota(jnp.int32, out_ref.shape, 1), owners)


def prepare(owners, tok_ref, ids_ref, codes_ref, expert_ref, out_ref):
    width = tok_ref.shape[1]
    rows = tok_ref.shape[0]
    top_count = ids_ref.shape[0]
    out_ref[:, :width] = tok_ref[...]
    ids = jnp.transpose(ids_ref[...])
    codes = jnp.transpose(codes_ref[...].astype(F32))
    shares = codes / jnp.sum(codes, axis=1, keepdims=True)
    lane = lax.broadcasted_iota(jnp.int32, (rows, LANES), 1)
    expert = expert_ref[...]
    dense = jnp.zeros((rows, LANES), F32)
    for k in range(top_count):
        dense += jnp.where(ids[:, k : k + 1] == expert, shares[:, k : k + 1], 0.0)
    high = dense.astype(BF16)
    low = (dense - high.astype(F32)).astype(BF16)
    out_ref[:, width:] = jnp.where(lane < owners, high, jnp.where(lane < 2 * owners, low, jnp.zeros_like(high)))


def stack(blocks, flops=0):
    def body(*refs):
        start = 0
        for ref in refs[:-1]:
            refs[-1][start : start + ref.shape[0], :] = ref[...]
            start += ref.shape[0]

    rows = sum(b.shape[0] for b in blocks)
    return call(body, jax.ShapeDtypeStruct((rows, blocks[0].shape[1]), BF16), *blocks, flops=flops)


def dot(a, b):
    return jnp.dot(a, b, preferred_element_type=F32)


def plus(*values):
    total = values[0].astype(F32)
    for value in values[1:]:
        total = total + value.astype(F32)
    return total


def half_rows(width, mine):
    half = lax.axis_index("tensor")
    start = half * width if mine else (1 - half) * width
    return pl.ds(pl.multiple_of(start, LANES), width)


def enter_own(owners, own, gate, up, gated, lifted, scale):
    rows = own.shape[0]
    width = own.shape[1] - LANES
    expert = lax.axis_index("dp") * lax.axis_size("expert") + lax.axis_index("expert")
    lane = lax.broadcasted_iota(jnp.int32, (rows, LANES), 1)
    mine = (lane == expert) | (lane == expert + owners)
    share = jnp.sum(jnp.where(mine, own[:, width:].astype(F32), 0.0), axis=1, keepdims=True)
    scale[...] = jnp.broadcast_to(share, (rows, LANES))
    at = half_rows(width, True)
    for weight, out in ((gate, gated), (up, lifted)):
        out[...] = dot(own[:, :width], weight[at, :])


def leave(at, scale, hidden, down, out):
    out[...] = (dot(hidden[...], down[:, at]) * scale[:, :1]).astype(BF16)


def enter_other(other, gate, up, down, gated, lifted, scale, hidden, send):
    width = send.shape[1]
    at = half_rows(width, False)
    for i in range(0, hidden.shape[1], TILE):
        there = pl.ds(i, TILE)
        g = gated[:, there] + dot(other[:, :width], gate[at, there])
        u = lifted[:, there] + dot(other[:, :width], up[at, there])
        hidden[:, there] = (jax.nn.silu(g) * u).astype(BF16)
    leave(at, scale, hidden, down, send)


def leave_own(hidden, down, scale, keep):
    leave(half_rows(keep.shape[1], True), scale, hidden, down, keep)


def dense(tokens, gate_weight, up_weight, down_weight, expert_ids, gate_codes):
    dp, ex = lax.axis_size("dp"), lax.axis_size("expert")
    owners = dp * ex
    n, width = tokens.shape[1:]
    units = gate_weight.shape[2]
    hops = range(1, ex)
    rows = ex * n

    def block(count):
        return jax.ShapeDtypeStruct((count, width), BF16)

    experts = call(functools.partial(table, owners), jax.ShapeDtypeStruct((n, LANES), jnp.int32), flops=STALL)
    first = call(
        functools.partial(prepare, owners),
        jax.ShapeDtypeStruct((n, width + LANES), BF16),
        tokens[0], expert_ids[0].T, gate_codes[0].T, experts,
    )
    line = {j: swap(first, "expert", j) for j in reversed(hops)}
    early = [first] + [line[j] for j in range(1, EARLY)]
    late = [line[j] for j in range(EARLY, ex)]
    parts_a = stack(early)
    parts_b = stack(late, flops=STALL)
    sent_a = {g: swap(parts_a, "dp", g) for g in range(1, dp)}
    sent_b = {g: swap(parts_b, "dp", g) for g in range(1, dp)}
    near = stack([parts_a, parts_b] + [sent_a[g] for g in range(1, dp)])
    far = stack([sent_b[g] for g in range(1, dp)])
    gate, up, down = gate_weight[0], up_weight[0], down_weight[0]

    def run(own):
        count = own.shape[0]
        floats = jax.ShapeDtypeStruct((count, units), F32)
        other = swap(own, "tensor", 1)
        gated, lifted, scale = call(
            functools.partial(enter_own, owners), [floats, floats, jax.ShapeDtypeStruct((count, LANES), F32)],
            own, gate, up, flops=HINT, limit=8,
        )
        hidden, send = call(
            enter_other, [jax.ShapeDtypeStruct((count, units), BF16), block(count)],
            other, gate, up, down, gated, lifted, scale, flops=HINT, limit=8,
        )
        keep = call(leave_own, block(count), hidden, down, scale, flops=HINT, limit=8)
        return keep, send

    keep_a, send_a = run(near)
    keep_b, send_b = run(far)
    recv_a = swap(send_a, "tensor", 1)
    recv_b = swap(send_b, "tensor", 1)
    cut = EARLY * n

    def add_far(keep_a, recv_a, keep_b, recv_b, x, y, *diag):
        for g, out in ((1, x), (2, y)):
            here, there = pl.ds(rows + (g - 1) * cut, cut), pl.ds((g - 1) * (rows - cut), rows - cut)
            out[:cut, :] = plus(keep_a[here, :], recv_a[here, :]).astype(BF16)
            out[cut:, :] = plus(keep_b[there, :], recv_b[there, :]).astype(BF16)
        for j, out in zip(hops, diag):
            if j < EARLY:
                keep, recv, here = keep_a, recv_a, pl.ds(rows + 2 * cut + j * n, n)
            else:
                keep, recv, here = keep_b, recv_b, pl.ds(2 * (rows - cut) + (j - EARLY) * n, n)
            out[...] = plus(keep[here, :], recv[here, :]).astype(BF16)

    x, y, *diag = call(add_far, [block(rows)] * 2 + [block(n)] * (ex - 1), keep_a, recv_a, keep_b, recv_b)
    sides = [swap(x, "dp", 1), swap(y, "dp", 2)]
    spread = [swap(diag[j - 1], "expert", j) for j in reversed(hops)]

    def add_diag(keep, recv, *rest):
        here = pl.ds(rows + 2 * cut, n)
        rest[-1][...] = plus(keep[here, :], recv[here, :], *[r[...] for r in rest[:-1]]).astype(BF16)

    def add_line(keep, recv, x, y, *outs):
        for i, out in enumerate(outs):
            there = pl.ds((i + 1) * n, n)
            out[...] = plus(keep[there, :], recv[there, :], x[there, :], y[there, :]).astype(BF16)

    lines = call(add_line, [block(n)] * (ex - 1), keep_a, recv_a, *sides)
    ends = [swap(lines[j - 1], "expert", j) for j in reversed(hops)]
    ends.append(swap(call(add_diag, block(n), keep_a, recv_a, *spread), "dp", 3))

    def add_end(keep, recv, x, y, *rest):
        here = pl.ds(0, n)
        rest[-1][...] = plus(keep[here, :], recv[here, :], x[here, :], y[here, :], *[r[...] for r in rest[:-1]]).astype(BF16)

    return call(add_end, block(n), keep_a, recv_a, *sides, *ends)[None]


def local(tokens, gate_weight, up_weight, down_weight, expert_ids, gate_codes):
    dp, ex = lax.axis_size("dp"), lax.axis_size("expert")
    owners = dp * ex
    tok_rows = tokens.shape[1]
    top_count = expert_ids.shape[2]
    slot_depth = min(tok_rows, max(2, 2 * tok_rows * top_count // owners))
    args = (tokens, gate_weight, up_weight, down_weight, expert_ids, gate_codes)
    grid = dp == 4 and ex & (ex - 1) == 0 and ex > 1 and lax.axis_size("tensor") == 2
    if slot_depth == tok_rows and grid and 2 * owners <= LANES:
        return dense(*args)
    return slotted(*args, slot_depth)


def solution(mesh):
    in_specs = (
        P(None, ("dp", "expert"), "tensor"),
        P(("dp", "expert"), None, "tensor"),
        P(("dp", "expert"), None, "tensor"),
        P(("dp", "expert"), "tensor", None),
        P(None, ("dp", "expert"), None),
        P(None, ("dp", "expert"), None),
    )
    out_specs = P(None, ("dp", "expert"), "tensor")
    return jax.shard_map(local, mesh=mesh, in_specs=in_specs, out_specs=out_specs, check_vma=False)
```

```python
import functools

import jax
import jax.numpy as jnp
from jax import lax
from jax.experimental import pallas as pl
from jax.experimental.pallas import tpu as pltpu
from jax.sharding import PartitionSpec as P


LANES = 128
SUBLANES = 8
STALL = 20000000000
EARLY = 2
TILE = 256
HINT = 2000000000


def slotted(tokens, gate_weight, up_weight, down_weight, expert_ids, gate_codes, slot_depth):
    owners = lax.axis_size("dp") * lax.axis_size("expert")
    tok_rows = tokens.shape[1]
    top_count = expert_ids.shape[2]
    slot_count = owners * slot_depth
    w_gate = gate_weight[0]
    w_up = up_weight[0]
    w_down = down_weight[0]
    slot_numbers = jnp.arange(slot_count, dtype=jnp.int32)
    owner_numbers = jnp.arange(owners, dtype=jnp.int32)
    step_tokens = tokens[0]
    route_ids = expert_ids[0].reshape(tok_rows * top_count)
    onehot = (route_ids[:, None] == owner_numbers[None, :]).astype(jnp.int32)
    before = jnp.cumsum(onehot, axis=0) - onehot
    slot_rank = jnp.sum(before * onehot, axis=1)
    slot_index = route_ids * slot_depth + slot_rank
    select = (slot_index[:, None] == slot_numbers[None, :]).astype(jnp.bfloat16)
    per_token = jnp.sum(select.reshape(tok_rows, top_count, slot_count), axis=1)
    packed = jnp.einsum(
        "ts,td->sd", per_token, step_tokens, preferred_element_type=jnp.float32
    ).astype(jnp.bfloat16)
    packed = packed.reshape(owners, slot_depth, step_tokens.shape[1])
    arrived = lax.all_to_all(packed, ("dp", "expert"), split_axis=0, concat_axis=0, tiled=True)
    owner_rows = arrived.reshape(slot_count, step_tokens.shape[1])
    owner_rows = lax.all_gather(owner_rows, "tensor", axis=1, tiled=True)
    gated = jnp.dot(owner_rows, w_gate, preferred_element_type=jnp.float32)
    lifted = jnp.dot(owner_rows, w_up, preferred_element_type=jnp.float32)
    hidden = (jax.nn.silu(gated) * lifted).astype(jnp.bfloat16)
    partial_value = jnp.dot(hidden, w_down, preferred_element_type=jnp.float32).astype(jnp.bfloat16)
    summed = (
        lax.psum_scatter(partial_value, "tensor", scatter_dimension=1, tiled=True)
        .astype(jnp.float32)
        .astype(jnp.bfloat16)
    )
    half_width = summed.shape[1]
    result = summed.reshape(owners, slot_depth, half_width)
    returned = lax.all_to_all(result, ("dp", "expert"), split_axis=0, concat_axis=0, tiled=True)
    returned = returned.reshape(slot_count, half_width)
    picked = jnp.dot(select, returned, preferred_element_type=jnp.float32)
    codes = gate_codes[0].astype(jnp.float32)
    shares = codes / jnp.sum(codes, axis=1, keepdims=True)
    mixed_rows = jnp.sum(
        picked.reshape(tok_rows, top_count, half_width) * shares[:, :, None], axis=1
    )
    return mixed_rows.astype(jnp.bfloat16)[None]


def swap(x, axis, offset):
    count = lax.axis_size(axis)
    return lax.ppermute(x, axis, [(i, i ^ offset) for i in range(count)])


VMEM = pl.BlockSpec(memory_space=pltpu.VMEM)
F32, BF16 = jnp.float32, jnp.bfloat16


def call(body, outs, *args, flops=0, scratch=(), limit=2):
    return pl.pallas_call(
        body,
        out_shape=outs,
        in_specs=[VMEM] * len(args),
        out_specs=jax.tree.map(lambda _: VMEM, outs),
        scratch_shapes=scratch,
        compiler_params=pltpu.CompilerParams(vmem_limit_bytes=limit * 2**20),
        cost_estimate=pl.CostEstimate(flops=flops, bytes_accessed=0, transcendentals=0),
    )(*args)


def table(owners, out_ref):
    out_ref[...] = lax.rem(lax.broadcasted_iota(jnp.int32, out_ref.shape, 1), owners)


def prepare(owners, tok_ref, ids_ref, codes_ref, expert_ref, out_ref):
    rows, width = tok_ref.shape
    top_count = ids_ref.shape[0]
    for i in range(width // LANES):
        out_ref[0, i * rows : (i + 1) * rows, :] = tok_ref[:, i * LANES : (i + 1) * LANES]
    ids = jnp.transpose(ids_ref[...])
    codes = jnp.transpose(codes_ref[...].astype(F32))
    shares = codes / jnp.sum(codes, axis=1, keepdims=True)
    lane = lax.broadcasted_iota(jnp.int32, (rows, LANES), 1)
    expert = expert_ref[...]
    dense = jnp.zeros((rows, LANES), F32)
    for k in range(top_count):
        dense += jnp.where(ids[:, k : k + 1] == expert, shares[:, k : k + 1], 0.0)
    high = dense.astype(BF16).astype(F32)
    both = jnp.where(lane < owners, high, dense - high)
    room = LANES * SUBLANES // rows
    tile = jnp.concatenate([both[t : t + SUBLANES, :room] for t in range(0, rows, SUBLANES)], axis=1)
    out_ref[0, rows * width // LANES :, :] = tile.astype(BF16)


def stack(blocks, flops=0):
    def body(*refs):
        start = 0
        for ref in refs[:-1]:
            refs[-1][start : start + ref.shape[0]] = ref[...]
            start += ref.shape[0]

    count = sum(b.shape[0] for b in blocks)
    return call(body, jax.ShapeDtypeStruct((count, *blocks[0].shape[1:]), BF16), *blocks, flops=flops)


def unpack(packed, x):
    n = x.shape[0] // packed.shape[0]
    for b in range(packed.shape[0]):
        for i in range(x.shape[1] // LANES):
            x[b * n : (b + 1) * n, i * LANES : (i + 1) * LANES] = packed[b, i * n : (i + 1) * n, :]


def dot(a, b):
    return jnp.dot(a, b, preferred_element_type=F32)


def plus(*values):
    total = values[0].astype(F32)
    for value in values[1:]:
        total = total + value.astype(F32)
    return total


def half_rows(width, mine):
    half = lax.axis_index("tensor")
    start = half * width if mine else (1 - half) * width
    return pl.ds(pl.multiple_of(start, LANES), width)


def enter_own(owners, own, gate, up, gated, lifted, scale, x):
    width = x.shape[1]
    n = x.shape[0] // own.shape[0]
    unpack(own, x)
    expert = lax.axis_index("dp") * lax.axis_size("expert") + lax.axis_index("expert")
    lane = lax.broadcasted_iota(jnp.int32, (SUBLANES, LANES), 1)
    for b in range(own.shape[0]):
        tile = own[b, n * width // LANES :, :].astype(F32)
        for t in range(0, n, SUBLANES):
            at = lane - t * LANES // n
            mine = (at == expert) | (at == expert + owners)
            share = jnp.sum(jnp.where(mine, tile, 0.0), axis=1, keepdims=True)
            scale[b * n + t : b * n + t + SUBLANES, :] = jnp.broadcast_to(share, (SUBLANES, LANES))
    at = half_rows(width, True)
    for weight, out in ((gate, gated), (up, lifted)):
        out[...] = dot(x[...], weight[at, :])


def leave(at, scale, hidden, down, out):
    out[...] = (dot(hidden[...], down[:, at]) * scale[:, :1]).astype(BF16)


def enter_other(other, gate, up, down, gated, lifted, scale, hidden, send, x):
    width = send.shape[1]
    unpack(other, x)
    at = half_rows(width, False)
    for i in range(0, hidden.shape[1], TILE):
        there = pl.ds(i, TILE)
        g = gated[:, there] + dot(x[...], gate[at, there])
        u = lifted[:, there] + dot(x[...], up[at, there])
        hidden[:, there] = (jax.nn.silu(g) * u).astype(BF16)
    leave(at, scale, hidden, down, send)


def leave_own(hidden, down, scale, keep):
    leave(half_rows(keep.shape[1], True), scale, hidden, down, keep)


def dense(tokens, gate_weight, up_weight, down_weight, expert_ids, gate_codes):
    dp, ex = lax.axis_size("dp"), lax.axis_size("expert")
    owners = dp * ex
    n, width = tokens.shape[1:]
    units = gate_weight.shape[2]
    hops = range(1, ex)
    rows = ex * n

    def block(count):
        return jax.ShapeDtypeStruct((count, width), BF16)

    experts = call(functools.partial(table, owners), jax.ShapeDtypeStruct((n, LANES), jnp.int32), flops=STALL)
    first = call(
        functools.partial(prepare, owners),
        jax.ShapeDtypeStruct((1, n * width // LANES + SUBLANES, LANES), BF16),
        tokens[0], expert_ids[0].T, gate_codes[0].T, experts,
    )
    line = {j: swap(first, "expert", j) for j in reversed(hops)}
    early = [first] + [line[j] for j in range(1, EARLY)]
    late = [line[j] for j in range(EARLY, ex)]
    parts_a = stack(early)
    parts_b = stack(late, flops=STALL)
    sent_a = {g: swap(parts_a if g < 3 else first, "dp", g) for g in range(1, dp)}
    turned = swap(sent_a[3], "expert", 1)
    sent_b = {g: swap(parts_b, "dp", g) for g in range(1, dp)}
    near = stack([parts_a, parts_b] + [sent_a[g] for g in range(1, dp)])
    far = stack([sent_b[g] for g in range(1, dp)] + [turned])
    gate, up, down = gate_weight[0], up_weight[0], down_weight[0]

    def run(own):
        count = own.shape[0] * n
        scratch = [pltpu.VMEM((count, width), BF16)]
        floats = jax.ShapeDtypeStruct((count, units), F32)
        other = swap(own, "tensor", 1)
        gated, lifted, scale = call(
            functools.partial(enter_own, owners), [floats, floats, jax.ShapeDtypeStruct((count, LANES), F32)],
            own, gate, up, flops=HINT, limit=8, scratch=scratch,
        )
        hidden, send = call(
            enter_other, [jax.ShapeDtypeStruct((count, units), BF16), block(count)],
            other, gate, up, down, gated, lifted, scale, flops=HINT, limit=8, scratch=scratch,
        )
        keep = call(leave_own, block(count), hidden, down, scale, flops=HINT, limit=8)
        return keep, send

    keep_a, send_a = run(near)
    keep_b, send_b = run(far)
    recv_a = swap(send_a, "tensor", 1)
    recv_b = swap(send_b, "tensor", 1)
    cut = EARLY * n

    def add_far(keep_a, recv_a, keep_b, recv_b, x, y, *diag):
        for g, out in ((1, x), (2, y)):
            here, there = pl.ds(rows + (g - 1) * cut, cut), pl.ds((g - 1) * (rows - cut), rows - cut)
            out[:cut, :] = plus(keep_a[here, :], recv_a[here, :]).astype(BF16)
            out[cut:, :] = plus(keep_b[there, :], recv_b[there, :]).astype(BF16)
        for j, out in zip(hops, diag):
            if j < EARLY:
                keep, recv, here = keep_b, recv_b, pl.ds((dp - 1) * (rows - cut) + (j - 1) * n, n)
            else:
                keep, recv, here = keep_b, recv_b, pl.ds(2 * (rows - cut) + (j - EARLY) * n, n)
            out[...] = plus(keep[here, :], recv[here, :]).astype(BF16)

    x, y, *diag = call(add_far, [block(rows)] * 2 + [block(n)] * (ex - 1), keep_a, recv_a, keep_b, recv_b)
    sides = [swap(x, "dp", 1), swap(y, "dp", 2)]
    spread = [swap(diag[j - 1], "expert", j) for j in reversed(hops)]

    def add_diag(keep, recv, *rest):
        here = pl.ds(rows + 2 * cut, n)
        rest[-1][...] = plus(keep[here, :], recv[here, :], *[r[...] for r in rest[:-1]]).astype(BF16)

    def add_line(keep, recv, x, y, *outs):
        for i, out in enumerate(outs):
            there = pl.ds((i + 1) * n, n)
            out[...] = plus(keep[there, :], recv[there, :], x[there, :], y[there, :]).astype(BF16)

    lines = call(add_line, [block(n)] * (ex - 1), keep_a, recv_a, *sides)
    ends = [swap(lines[j - 1], "expert", j) for j in reversed(hops)]
    ends.append(swap(call(add_diag, block(n), keep_a, recv_a, *spread), "dp", 3))

    def add_end(keep, recv, x, y, *rest):
        here = pl.ds(0, n)
        rest[-1][...] = plus(keep[here, :], recv[here, :], x[here, :], y[here, :], *[r[...] for r in rest[:-1]]).astype(BF16)

    return call(add_end, block(n), keep_a, recv_a, *sides, *ends)[None]


def local(tokens, gate_weight, up_weight, down_weight, expert_ids, gate_codes):
    dp, ex = lax.axis_size("dp"), lax.axis_size("expert")
    owners = dp * ex
    tok_rows = tokens.shape[1]
    top_count = expert_ids.shape[2]
    slot_depth = min(tok_rows, max(2, 2 * tok_rows * top_count // owners))
    args = (tokens, gate_weight, up_weight, down_weight, expert_ids, gate_codes)
    grid = dp == 4 and ex & (ex - 1) == 0 and ex > 1 and lax.axis_size("tensor") == 2
    if slot_depth == tok_rows and grid and tok_rows % SUBLANES == 0 and 2 * owners * tok_rows <= LANES * SUBLANES:
        return dense(*args)
    return slotted(*args, slot_depth)


def solution(mesh):
    in_specs = (
        P(None, ("dp", "expert"), "tensor"),
        P(("dp", "expert"), None, "tensor"),
        P(("dp", "expert"), None, "tensor"),
        P(("dp", "expert"), "tensor", None),
        P(None, ("dp", "expert"), None),
        P(None, ("dp", "expert"), None),
    )
    out_specs = P(None, ("dp", "expert"), "tensor")
    return jax.shard_map(local, mesh=mesh, in_specs=in_specs, out_specs=out_specs, check_vma=False)
```

```python
import functools

import jax
import jax.numpy as jnp
from jax import lax
from jax.experimental import pallas as pl
from jax.experimental.pallas import tpu as pltpu
from jax.sharding import PartitionSpec as P


LANES = 128
SUBLANES = 8
STALL = 20000000000
EARLY = 2
TILE = 256
HINT = 2000000000


def slotted(tokens, gate_weight, up_weight, down_weight, expert_ids, gate_codes, slot_depth):
    owners = lax.axis_size("dp") * lax.axis_size("expert")
    tok_rows = tokens.shape[1]
    top_count = expert_ids.shape[2]
    slot_count = owners * slot_depth
    w_gate = gate_weight[0]
    w_up = up_weight[0]
    w_down = down_weight[0]
    slot_numbers = jnp.arange(slot_count, dtype=jnp.int32)
    owner_numbers = jnp.arange(owners, dtype=jnp.int32)
    step_tokens = tokens[0]
    route_ids = expert_ids[0].reshape(tok_rows * top_count)
    onehot = (route_ids[:, None] == owner_numbers[None, :]).astype(jnp.int32)
    before = jnp.cumsum(onehot, axis=0) - onehot
    slot_rank = jnp.sum(before * onehot, axis=1)
    slot_index = route_ids * slot_depth + slot_rank
    select = (slot_index[:, None] == slot_numbers[None, :]).astype(jnp.bfloat16)
    per_token = jnp.sum(select.reshape(tok_rows, top_count, slot_count), axis=1)
    packed = jnp.einsum(
        "ts,td->sd", per_token, step_tokens, preferred_element_type=jnp.float32
    ).astype(jnp.bfloat16)
    packed = packed.reshape(owners, slot_depth, step_tokens.shape[1])
    arrived = lax.all_to_all(packed, ("dp", "expert"), split_axis=0, concat_axis=0, tiled=True)
    owner_rows = arrived.reshape(slot_count, step_tokens.shape[1])
    owner_rows = lax.all_gather(owner_rows, "tensor", axis=1, tiled=True)
    gated = jnp.dot(owner_rows, w_gate, preferred_element_type=jnp.float32)
    lifted = jnp.dot(owner_rows, w_up, preferred_element_type=jnp.float32)
    hidden = (jax.nn.silu(gated) * lifted).astype(jnp.bfloat16)
    partial_value = jnp.dot(hidden, w_down, preferred_element_type=jnp.float32).astype(jnp.bfloat16)
    summed = (
        lax.psum_scatter(partial_value, "tensor", scatter_dimension=1, tiled=True)
        .astype(jnp.float32)
        .astype(jnp.bfloat16)
    )
    half_width = summed.shape[1]
    result = summed.reshape(owners, slot_depth, half_width)
    returned = lax.all_to_all(result, ("dp", "expert"), split_axis=0, concat_axis=0, tiled=True)
    returned = returned.reshape(slot_count, half_width)
    picked = jnp.dot(select, returned, preferred_element_type=jnp.float32)
    codes = gate_codes[0].astype(jnp.float32)
    shares = codes / jnp.sum(codes, axis=1, keepdims=True)
    mixed_rows = jnp.sum(
        picked.reshape(tok_rows, top_count, half_width) * shares[:, :, None], axis=1
    )
    return mixed_rows.astype(jnp.bfloat16)[None]


def swap(x, axis, offset):
    count = lax.axis_size(axis)
    return lax.ppermute(x, axis, [(i, i ^ offset) for i in range(count)])


VMEM = pl.BlockSpec(memory_space=pltpu.VMEM)
F32, BF16 = jnp.float32, jnp.bfloat16


def call(body, outs, *args, flops=0, scratch=(), limit=2):
    return pl.pallas_call(
        body,
        out_shape=outs,
        in_specs=[VMEM] * len(args),
        out_specs=jax.tree.map(lambda _: VMEM, outs),
        scratch_shapes=scratch,
        compiler_params=pltpu.CompilerParams(vmem_limit_bytes=limit * 2**20),
        cost_estimate=pl.CostEstimate(flops=flops, bytes_accessed=0, transcendentals=0),
    )(*args)


def table(owners, out_ref):
    out_ref[...] = lax.rem(lax.broadcasted_iota(jnp.int32, out_ref.shape, 1), owners)


def prepare(owners, tok_ref, ids_ref, codes_ref, expert_ref, out_ref):
    rows, width = tok_ref.shape
    top_count = ids_ref.shape[0]
    for i in range(width // LANES):
        out_ref[0, i * rows : (i + 1) * rows, :] = tok_ref[:, i * LANES : (i + 1) * LANES]
    ids = jnp.transpose(ids_ref[...])
    codes = jnp.transpose(codes_ref[...].astype(F32))
    shares = codes / jnp.sum(codes, axis=1, keepdims=True)
    lane = lax.broadcasted_iota(jnp.int32, (rows, LANES), 1)
    expert = expert_ref[...]
    dense = jnp.zeros((rows, LANES), F32)
    for k in range(top_count):
        dense += jnp.where(ids[:, k : k + 1] == expert, shares[:, k : k + 1], 0.0)
    high = dense.astype(BF16).astype(F32)
    both = jnp.where(lane < owners, high, dense - high)
    room = LANES * SUBLANES // rows
    tile = jnp.concatenate([both[t : t + SUBLANES, :room] for t in range(0, rows, SUBLANES)], axis=1)
    out_ref[0, rows * width // LANES :, :] = tile.astype(BF16)


def stack(blocks, flops=0):
    def body(*refs):
        start = 0
        for ref in refs[:-1]:
            refs[-1][start : start + ref.shape[0]] = ref[...]
            start += ref.shape[0]

    count = sum(b.shape[0] for b in blocks)
    return call(body, jax.ShapeDtypeStruct((count, *blocks[0].shape[1:]), BF16), *blocks, flops=flops)


def unpack(packed, x):
    n = x.shape[0] // packed.shape[0]
    for b in range(packed.shape[0]):
        for i in range(x.shape[1] // LANES):
            x[b * n : (b + 1) * n, i * LANES : (i + 1) * LANES] = packed[b, i * n : (i + 1) * n, :]


def dot(a, b):
    return jnp.dot(a, b, preferred_element_type=F32)


def plus(*values):
    total = values[0].astype(F32)
    for value in values[1:]:
        total = total + value.astype(F32)
    return total


def half_rows(width, mine):
    half = lax.axis_index("tensor")
    start = half * width if mine else (1 - half) * width
    return pl.ds(pl.multiple_of(start, LANES), width)


def enter_own(owners, own, gate, up, gated, lifted, scale, x):
    width = x.shape[1]
    n = x.shape[0] // own.shape[0]
    unpack(own, x)
    expert = lax.axis_index("dp") * lax.axis_size("expert") + lax.axis_index("expert")
    lane = lax.broadcasted_iota(jnp.int32, (SUBLANES, LANES), 1)
    for b in range(own.shape[0]):
        tile = own[b, n * width // LANES :, :].astype(F32)
        for t in range(0, n, SUBLANES):
            at = lane - t * LANES // n
            mine = (at == expert) | (at == expert + owners)
            share = jnp.sum(jnp.where(mine, tile, 0.0), axis=1, keepdims=True)
            scale[b * n + t : b * n + t + SUBLANES, :] = jnp.broadcast_to(share, (SUBLANES, LANES))
    at = half_rows(width, True)
    for weight, out in ((gate, gated), (up, lifted)):
        out[...] = dot(x[...], weight[at, :])


def leave(at, scale, hidden, down, outs):
    value = dot(hidden[...], down[:, at]) * scale[:, :1]
    start = 0
    for out in outs:
        out[...] = value[start : start + out.shape[0]].astype(BF16)
        start += out.shape[0]


def enter_other(other, gate, up, down, gated, lifted, scale, hidden, *refs):
    send, x = refs[:-1], refs[-1]
    width = x.shape[1]
    unpack(other, x)
    at = half_rows(width, False)
    for i in range(0, hidden.shape[1], TILE):
        there = pl.ds(i, TILE)
        g = gated[:, there] + dot(x[...], gate[at, there])
        u = lifted[:, there] + dot(x[...], up[at, there])
        hidden[:, there] = (jax.nn.silu(g) * u).astype(BF16)
    leave(at, scale, hidden, down, send)


def leave_own(hidden, down, scale, keep):
    leave(half_rows(keep.shape[1], True), scale, hidden, down, [keep])


def dense(tokens, gate_weight, up_weight, down_weight, expert_ids, gate_codes):
    dp, ex = lax.axis_size("dp"), lax.axis_size("expert")
    owners = dp * ex
    n, width = tokens.shape[1:]
    units = gate_weight.shape[2]
    hops = range(1, ex)
    rows = ex * n

    def block(count):
        return jax.ShapeDtypeStruct((count, width), BF16)

    experts = call(functools.partial(table, owners), jax.ShapeDtypeStruct((n, LANES), jnp.int32), flops=STALL)
    first = call(
        functools.partial(prepare, owners),
        jax.ShapeDtypeStruct((1, n * width // LANES + SUBLANES, LANES), BF16),
        tokens[0], expert_ids[0].T, gate_codes[0].T, experts,
    )
    line = {j: swap(first, "expert", j) for j in reversed(hops)}
    early = [first] + [line[j] for j in range(1, EARLY)]
    late = [line[j] for j in range(EARLY, ex)]
    parts_a = stack(early)
    parts_b = stack(late, flops=STALL)
    sent_a = {g: swap(parts_a if g < 3 else first, "dp", g) for g in range(1, dp)}
    turned = swap(sent_a[3], "expert", 1)
    sent_b = {g: swap(parts_b, "dp", g) for g in range(1, dp)}
    near = stack([parts_a, parts_b] + [sent_a[g] for g in range(1, dp)])
    far = stack([sent_b[g] for g in range(1, dp)] + [turned])
    gate, up, down = gate_weight[0], up_weight[0], down_weight[0]

    def run(own, cuts):
        count = own.shape[0] * n
        scratch = [pltpu.VMEM((count, width), BF16)]
        floats = jax.ShapeDtypeStruct((count, units), F32)
        other = swap(own, "tensor", 1)
        gated, lifted, scale = call(
            functools.partial(enter_own, owners), [floats, floats, jax.ShapeDtypeStruct((count, LANES), F32)],
            own, gate, up, flops=HINT, limit=8, scratch=scratch,
        )
        hidden, *send = call(
            enter_other, [jax.ShapeDtypeStruct((count, units), BF16)] + [block(part) for part in cuts],
            other, gate, up, down, gated, lifted, scale, flops=HINT, limit=8, scratch=scratch,
        )
        keep = call(leave_own, block(count), hidden, down, scale, flops=HINT, limit=8)
        return keep, send

    sums = 2 * (ex - EARLY) * n
    keep_a, (send_a,) = run(near, [near.shape[0] * n])
    keep_b, (send_b, send_d) = run(far, [sums, far.shape[0] * n - sums])
    recv_a = swap(send_a, "tensor", 1)
    recv_b = swap(send_b, "tensor", 1)
    recv_d = swap(send_d, "tensor", 1)
    cut = EARLY * n

    def add_far(keep_a, recv_a, keep_b, recv_b, x, y):
        for g, out in ((1, x), (2, y)):
            here, there = pl.ds(rows + (g - 1) * cut, cut), pl.ds((g - 1) * (rows - cut), rows - cut)
            out[:cut, :] = plus(keep_a[here, :], recv_a[here, :]).astype(BF16)
            out[cut:, :] = plus(keep_b[there, :], recv_b[there, :]).astype(BF16)

    def add_turned(keep_b, recv_d, *diag):
        for j, out in zip(hops, diag):
            start = (j - EARLY) * n if j >= EARLY else rows - cut + (j - 1) * n
            out[...] = plus(keep_b[pl.ds(sums + start, n), :], recv_d[pl.ds(start, n), :]).astype(BF16)

    x, y = call(add_far, [block(rows)] * 2, keep_a, recv_a, keep_b, recv_b)
    diag = call(add_turned, [block(n)] * (ex - 1), keep_b, recv_d)
    sides = [swap(x, "dp", 1), swap(y, "dp", 2)]
    spread = [swap(diag[j - 1], "expert", j) for j in reversed(hops)]

    def add_diag(keep, recv, *rest):
        here = pl.ds(rows + 2 * cut, n)
        rest[-1][...] = plus(keep[here, :], recv[here, :], *[r[...] for r in rest[:-1]]).astype(BF16)

    def add_line(keep, recv, x, y, *outs):
        for i, out in enumerate(outs):
            there = pl.ds((i + 1) * n, n)
            out[...] = plus(keep[there, :], recv[there, :], x[there, :], y[there, :]).astype(BF16)

    lines = call(add_line, [block(n)] * (ex - 1), keep_a, recv_a, *sides)
    ends = [swap(lines[j - 1], "expert", j) for j in reversed(hops)]
    ends.append(swap(call(add_diag, block(n), keep_a, recv_a, *spread), "dp", 3))

    def add_end(keep, recv, x, y, *rest):
        here = pl.ds(0, n)
        rest[-1][...] = plus(keep[here, :], recv[here, :], x[here, :], y[here, :], *[r[...] for r in rest[:-1]]).astype(BF16)

    return call(add_end, block(n), keep_a, recv_a, *sides, *ends)[None]


def local(tokens, gate_weight, up_weight, down_weight, expert_ids, gate_codes):
    dp, ex = lax.axis_size("dp"), lax.axis_size("expert")
    owners = dp * ex
    tok_rows = tokens.shape[1]
    top_count = expert_ids.shape[2]
    slot_depth = min(tok_rows, max(2, 2 * tok_rows * top_count // owners))
    args = (tokens, gate_weight, up_weight, down_weight, expert_ids, gate_codes)
    grid = dp == 4 and ex & (ex - 1) == 0 and ex > 1 and lax.axis_size("tensor") == 2
    if slot_depth == tok_rows and grid and tok_rows % SUBLANES == 0 and 2 * owners * tok_rows <= LANES * SUBLANES:
        return dense(*args)
    return slotted(*args, slot_depth)


def solution(mesh):
    in_specs = (
        P(None, ("dp", "expert"), "tensor"),
        P(("dp", "expert"), None, "tensor"),
        P(("dp", "expert"), None, "tensor"),
        P(("dp", "expert"), "tensor", None),
        P(None, ("dp", "expert"), None),
        P(None, ("dp", "expert"), None),
    )
    out_specs = P(None, ("dp", "expert"), "tensor")
    return jax.shard_map(local, mesh=mesh, in_specs=in_specs, out_specs=out_specs, check_vma=False)
```
